8 devices in a mesh: dp: 1 (over z), tp: 8 (over y, x, core).
Axes of the slice: x: 2, y: 2, z: 1, core: 2. Of those that a mesh axis runs over, the one named last changes fastest.
Arguments:
- enc_out: bfloat16 [12, 2048, 1024], P('dp', 'tp')
- norm_scale: bfloat16 [1024], replicated
- w_key: bfloat16 [3, 1024, 32, 128], P(None, None, 'tp')
- w_value: bfloat16 [3, 1024, 32, 128], P(None, None, 'tp')
Outputs:
- output 1: bfloat16 [3, 12, 2048, 32, 128], P(None, 'dp', None, 'tp')
- output 2: bfloat16 [3, 12, 2048, 32, 128], P(None, 'dp', None, 'tp')
All inputs are finite; a program needn't handle non-finite values.
Results may differ from the reference program's by a relative error of at most 0.001.
Values are sent between devices in bfloat16 or wider.
A program may use at most 1 GiB of HBM per device.

```python
import jax
import jax.numpy as jnp
from jax import lax

N_LAYERS = 3
BATCH_SIZE = 12
SEQ_LEN = 2048
D_MODEL = 1024
N_HEADS = 32
HEAD_DIM = 128
NORM_EPS = 1e-6


def setup_inputs(seed: int = 0, part: int = 0) -> dict:
    root_key = jax.random.key(seed)
    k_act, k_norm, k_key, k_val = jax.random.split(root_key, 4)
    k_act = jax.random.fold_in(k_act, part)
    w_scale = D_MODEL ** -0.5
    w_shape = (N_LAYERS, D_MODEL, N_HEADS, HEAD_DIM)
    enc_out = jax.random.normal(k_act, (BATCH_SIZE, SEQ_LEN, D_MODEL), jnp.float32)
    norm_scale = jax.random.uniform(k_norm, (D_MODEL,), jnp.float32, 0.5, 1.5)
    w_key = jax.random.normal(k_key, w_shape, jnp.float32) * w_scale
    w_value = jax.random.normal(k_val, w_shape, jnp.float32) * w_scale
    return {"enc_out": enc_out.astype(jnp.bfloat16), "norm_scale": norm_scale.astype(jnp.bfloat16), "w_key": w_key.astype(jnp.bfloat16), "w_value": w_value.astype(jnp.bfloat16)}


def rms_norm(enc_out, norm_scale):
    acts = enc_out.astype(jnp.float32)
    mean_sq = jnp.mean(acts * acts, axis=-1, keepdims=True)
    return (acts * lax.rsqrt(mean_sq + NORM_EPS) * norm_scale.astype(jnp.float32)).astype(jnp.bfloat16)


def reference(enc_out, norm_scale, w_key, w_value):
    normed = rms_norm(enc_out, norm_scale).reshape(BATCH_SIZE * SEQ_LEN, D_MODEL)
    out_shape = (BATCH_SIZE, SEQ_LEN, N_HEADS, HEAD_DIM)

    def project(layer_weights):
        layer_key, layer_value = layer_weights
        keys = jnp.dot(normed, layer_key.reshape(D_MODEL, N_HEADS * HEAD_DIM), preferred_element_type=jnp.float32)
        values = jnp.dot(normed, layer_value.reshape(D_MODEL, N_HEADS * HEAD_DIM), preferred_element_type=jnp.float32)
        return keys.astype(jnp.bfloat16).reshape(out_shape), values.astype(jnp.bfloat16).reshape(out_shape)

    key_cache, value_cache = lax.map(project, (w_key, w_value))
    return key_cache, value_cache
```

```python
import functools

import jax
import jax.numpy as jnp
from jax import lax
from jax.experimental import pallas as pl
from jax.experimental.pallas import tpu as pltpu
from jax.sharding import PartitionSpec as P


NORM_EPS = 1e-6

CORE, NEAR_X, NEAR_Y, DIAGONAL = 1, 2, 4, 6
BATCHES_PER_UNIT = 2
PIECES = (4, 2)
ORDER = ("a0", "b0", "a1", "f0", "b1", "f1")

HBM = pl.BlockSpec(memory_space=pltpu.HBM)
VMEM = pl.BlockSpec(memory_space=pltpu.VMEM)


def rms_norm(enc_out, norm_scale):
    acts = enc_out.astype(jnp.float32)
    mean_sq = jnp.mean(acts * acts, axis=-1, keepdims=True)
    return (acts * lax.rsqrt(mean_sq + NORM_EPS) * norm_scale.astype(jnp.float32)).astype(jnp.bfloat16)


def norm_kernel(*refs):
    n = len(refs) // 2
    for x_ref, y_ref in zip(refs[:n], refs[n + 1 :]):
        y_ref[...] = rms_norm(x_ref[...], refs[n][...])


def normalize(enc_out, norm_scale, first, n):
    _, seq, width = enc_out.shape
    return pl.pallas_call(
        norm_kernel,
        out_shape=[jax.ShapeDtypeStruct((n, seq, width), jnp.bfloat16) for _ in first],
        grid=(n,),
        in_specs=[pl.BlockSpec((1, seq, width), functools.partial(lambda f, i: (f + i, 0, 0), f)) for f in first]
        + [pl.BlockSpec((1, width), lambda i: (0, 0))],
        out_specs=[pl.BlockSpec((1, seq, width), lambda i: (i, 0, 0)) for _ in first],
        cost_estimate=pl.CostEstimate(flops=8 * len(first) * n * seq * width, bytes_accessed=4 * len(first) * n * seq * width, transcendentals=0),
        name="normalize",
    )(*[enc_out] * len(first), norm_scale.reshape(1, width))


def together(*values):
    return lax.optimization_barrier(values)


def pick(n, values):
    out = values[-1]
    for k in range(len(values) - 2, -1, -1):
        out = jnp.where(n == k, values[k], out)
    return out


def project_kernel(plan, n_layers, *refs):
    n_arrays, group = len(plan), BATCHES_PER_UNIT
    arrays, weights = refs[:n_arrays], refs[n_arrays : n_arrays + 2]
    *outs, tokens, rounded, in_sem, out_sem = refs[-6:]
    seq = arrays[0].shape[1]
    rows = rounded.shape[2] // group
    me = lax.axis_index("tp")
    flat = [(a, e, first + e, mask) for a, (n, first, mask) in enumerate(plan) for e in range(n)]
    units = [flat[k : k + group] for k in range(0, len(flat), group)]

    def load(n, slot):
        for k, unit in enumerate(units):

            @pl.when(n == k)
            def _():
                for g, (a, e, _, _) in enumerate(unit):
                    pltpu.make_async_copy(arrays[a].at[e], tokens.at[slot, pl.ds(g * seq, seq)], in_sem.at[slot, g]).start()

    def stores(n, slot):
        for g in range(group):
            entry = pick(n, [unit[g][2] for unit in units])
            source = me ^ pick(n, [unit[g][3] for unit in units])
            for j in range(2 * n_layers):
                to = outs[j % 2].at[j // 2, entry, pl.ds(pl.multiple_of(source * rows, rows), rows)]
                yield pltpu.make_async_copy(rounded.at[slot, j, pl.ds(g * rows, rows)], to, out_sem.at[slot, j, g])

    load(0, 0)

    def body(n, _):
        slot = lax.rem(n, 2)
        for g in range(group):
            pltpu.make_async_copy(arrays[0].at[0], tokens.at[slot, pl.ds(g * seq, seq)], in_sem.at[slot, g]).wait()

        @pl.when(n + 1 < len(units))
        def _():
            load(n + 1, 1 - slot)

        @pl.when(n >= 2)
        def _():
            for copy in stores(n, slot):
                copy.wait()

        x = tokens[slot]
        for j in range(2 * n_layers):
            product = jnp.dot(x, weights[j % 2][j // 2], preferred_element_type=jnp.float32)
            rounded[slot, j] = product.reshape(rounded.shape[2:]).astype(jnp.bfloat16)
        for copy in stores(n, slot):
            copy.start()
        return 0

    lax.fori_loop(0, len(units), body, 0)
    for n in range(max(len(units) - 2, 0), len(units)):
        for copy in stores(n, n % 2):
            copy.wait()


def project(arrays, plan, weights, caches, cache_shape):
    n_arrays, group = len(arrays), BATCHES_PER_UNIT
    n_layers, width, columns = weights[0].shape
    seq = arrays[0].shape[1]
    rows, lanes = group * seq * columns // 128, 128
    entries = sum(n for n, _, _ in plan)
    arrays = [pltpu.with_memory_space_constraint(a, pltpu.HBM) for a in arrays]
    weights = [pltpu.with_memory_space_constraint(w, pltpu.VMEM) for w in weights]
    return pl.pallas_call(
        functools.partial(project_kernel, plan, n_layers),
        out_shape=[jax.ShapeDtypeStruct(cache_shape, jnp.bfloat16)] * 2,
        in_specs=[HBM] * n_arrays + [VMEM, VMEM] + [HBM] * len(caches),
        out_specs=[HBM, HBM],
        input_output_aliases={n_arrays + 2 + i: i for i in range(len(caches))},
        scratch_shapes=[
            pltpu.VMEM((2, group * seq, width), jnp.bfloat16),
            pltpu.VMEM((2, 2 * n_layers, rows, lanes), jnp.bfloat16),
            pltpu.SemaphoreType.DMA((2, group)),
            pltpu.SemaphoreType.DMA((2, 2 * n_layers, group)),
        ],
        compiler_params=pltpu.CompilerParams(vmem_limit_bytes=57 * 2**20),
        cost_estimate=pl.CostEstimate(
            flops=2 * entries * seq * width * columns * 2 * n_layers,
            bytes_accessed=2 * entries * seq * (width + columns * 2 * n_layers),
            transcendentals=0,
        ),
    )(*arrays, *weights, *caches)


def solution(mesh):
    def per_device(enc_out, norm_scale, w_key, w_value):
        n_batch, seq, width = enc_out.shape
        n_layers, _, heads, head_dim = w_key.shape
        n_dev = mesh.shape["tp"]

        def swap(a, mask):
            return lax.ppermute(a, "tp", [(i, i ^ mask) for i in range(n_dev)])

        first = [sum(PIECES[:k]) for k in range(len(PIECES))]
        half = sum(PIECES)
        own, spans = ([], []), ([], [])
        for f, n in zip(first, PIECES):
            for s, y in enumerate(normalize(enc_out, norm_scale, (f, half + f), n)):
                own[s].append(y)
                spans[s].append((n, s * half + f))

        arrived = {}

        def send(what):
            for link, mask in ((0, NEAR_X), (1, NEAR_Y)):
                kind, k = what[0], int(what[1])
                if kind == "f":
                    array, span, _ = arrived[1 - link, f"a{k}"]
                    arrived[link, what] = [swap(array, mask), span, DIAGONAL]
                else:
                    s = link if kind == "a" else 1 - link
                    arrived[link, what] = [swap(own[s][k], mask), spans[s][k], mask]

        def to_partner(group):
            return [[swap(a, CORE), span, mask ^ CORE] for a, span, mask in group]

        for what in ORDER:
            if what[0] != "f":
                send(what)
        mine = [[own[s][k], spans[s][k], 0] for s in (0, 1) for k in range(len(PIECES))]
        theirs = to_partner(mine)
        *_, w_key, w_value = together(*[y for ys in own for y in ys], w_key, w_value)
        weights = [w.reshape(n_layers, width, heads * head_dim) for w in (w_key, w_value)]
        cache_shape, caches = (n_layers, n_batch, n_dev * seq * heads, head_dim), ()

        def call(group, caches):
            return project([a for a, _, _ in group], [(*span, mask) for _, span, mask in group], weights, caches, cache_shape)

        caches = call(mine, caches)
        caches = call(theirs, caches)
        waiting = []
        for what in ORDER:
            group = [arrived[link, what] for link in (0, 1)]
            group[0][0], group[1][0], *caches = together(group[0][0], group[1][0], *caches)
            if what[0] == "a":
                send("f" + what[1])
            to_come = to_partner(group)
            caches = call(waiting + group, caches)
            waiting = to_come
        caches = call(waiting, caches)
        return tuple(c.reshape(n_layers, n_batch, n_dev * seq, heads, head_dim) for c in caches)

    weight_spec = P(None, None, "tp", None)
    cache_spec = P(None, "dp", None, "tp", None)
    return jax.shard_map(per_device, mesh=mesh, in_specs=(P("dp", "tp", None), P(None), weight_spec, weight_spec), out_specs=(cache_spec, cache_spec), check_vma=False)
```

```python
import functools

import jax
import jax.numpy as jnp
from jax import lax
from jax.experimental import pallas as pl
from jax.experimental.pallas import tpu as pltpu
from jax.sharding import PartitionSpec as P


NORM_EPS = 1e-6

CORE, NEAR_X, NEAR_Y, DIAGONAL = 1, 2, 4, 6
PIECES = (4, 2)
ORDER = ("a0", "b0", "f0", "a1", "b1", "f1")
JOINED = ("a0",)

HBM = pl.BlockSpec(memory_space=pltpu.HBM)
VMEM = pl.BlockSpec(memory_space=pltpu.VMEM)


def rms_norm(enc_out, norm_scale):
    acts = enc_out.astype(jnp.float32)
    mean_sq = jnp.mean(acts * acts, axis=-1, keepdims=True)
    return (acts * lax.rsqrt(mean_sq + NORM_EPS) * norm_scale.astype(jnp.float32)).astype(jnp.bfloat16)


def prepare_kernel(pieces, has_weights, *refs):
    enc_out, norm_scale, *refs = refs
    entries = [(p, e, first + e) for p, (first, n) in enumerate(pieces) for e in range(n)]
    if has_weights:
        w_in, refs = refs[:2], refs[2:]
    outs, refs = refs[: len(pieces)], refs[len(pieces) :]
    if has_weights:
        w_out, refs = refs[:2], refs[2:]
    x, y, scale, in_sem, out_sem, scale_sem, *refs = refs
    load_scale = pltpu.make_async_copy(norm_scale, scale, scale_sem)
    load_scale.start()
    loads = [pltpu.make_async_copy(enc_out.at[b], x.at[k], in_sem.at[k]) for k, (_, _, b) in enumerate(entries)]
    stores = [pltpu.make_async_copy(y.at[k], outs[p].at[e], out_sem.at[k]) for k, (p, e, _) in enumerate(entries)]
    for copy in loads:
        copy.start()
    w_loads = []
    if has_weights:
        w_raw, w_sem = refs
        n_layers = w_raw.shape[1]
        w_loads = [(i, l, pltpu.make_async_copy(w_in[i].at[l], w_raw.at[i, l], w_sem.at[i, l])) for l in range(n_layers) for i in (0, 1)]
    for _, _, copy in w_loads:
        copy.start()
    load_scale.wait()

    def normalize(k, _):
        pltpu.make_async_copy(enc_out.at[0], x.at[k], in_sem.at[k]).wait()
        y[k] = rms_norm(x[k], scale[...])
        for i, store in enumerate(stores):

            @pl.when(k == i)
            def _():
                store.start()

        return 0

    lax.fori_loop(0, len(entries), normalize, 0)
    if has_weights:

        def lay_out(l, _):
            for i in (0, 1):
                pltpu.make_async_copy(w_in[i].at[l], w_raw.at[i, l], w_sem.at[i, l]).wait()
                w_out[i][l] = w_raw[i, l].reshape(w_out[i].shape[1:])
            return 0

        lax.fori_loop(0, n_layers, lay_out, 0)
    for store in stores:
        store.wait()


def prepare(enc_out, norm_scale, pieces, weights=()):
    _, seq, width = enc_out.shape
    n = sum(n for _, n in pieces)
    out_shape = [jax.ShapeDtypeStruct((n, seq, width), jnp.bfloat16) for _, n in pieces]
    scratch = [pltpu.VMEM((n, seq, width), jnp.bfloat16)] * 2 + [pltpu.VMEM((width,), jnp.bfloat16)]
    scratch += [pltpu.SemaphoreType.DMA((n,))] * 2 + [pltpu.SemaphoreType.DMA]
    for w in weights[:1]:
        n_layers, _, heads, head_dim = w.shape
        out_shape += [jax.ShapeDtypeStruct((n_layers, width, heads * head_dim), jnp.bfloat16)] * 2
        scratch += [pltpu.VMEM((2, *w.shape), jnp.bfloat16), pltpu.SemaphoreType.DMA((2, n_layers))]
    return pl.pallas_call(
        functools.partial(prepare_kernel, pieces, bool(weights)),
        out_shape=out_shape,
        in_specs=[HBM] * (2 + len(weights)),
        out_specs=[HBM] * len(pieces) + [VMEM] * len(weights),
        scratch_shapes=scratch,
        compiler_params=pltpu.CompilerParams(vmem_limit_bytes=(32 if weights else 57) * 2**20),
        cost_estimate=pl.CostEstimate(flops=8 * n * seq * width, bytes_accessed=4 * n * seq * width, transcendentals=0),
    )(*[pltpu.with_memory_space_constraint(a, pltpu.HBM) for a in (enc_out, norm_scale, *weights)])


def together(*values):
    return lax.optimization_barrier(values)


def pick(n, values):
    out = values[-1]
    for k in range(len(values) - 2, -1, -1):
        out = jnp.where(n == k, values[k], out)
    return out


def multiply_unit(x, weights, rounded, slot, stores):
    for j in range(rounded.shape[1]):
        product = jnp.dot(x, weights[j % 2][j // 2], preferred_element_type=jnp.float32)
        rounded[slot, j] = product.reshape(rounded.shape[2:]).astype(jnp.bfloat16)
        for copy in stores([j]):
            copy.start()


def unit_stores(rounded, outs, sem, slot, places, matrices):
    rows = rounded.shape[2] // len(places)
    for g, (entry, source) in enumerate(places):
        for j in matrices:
            to = outs[j % 2].at[j // 2, entry, pl.ds(pl.multiple_of(source * rows, rows), rows)]
            yield pltpu.make_async_copy(rounded.at[slot, j, pl.ds(g * rows, rows)], to, sem.at[slot, j, g])


def run_units(n_units, prefetch, tokens, weights, outs, rounded, sem, places):
    every = range(rounded.shape[1])

    def body(n, _):
        slot = lax.rem(n, 2)
        prefetch(n, slot)

        @pl.when(n >= 2)
        def _():
            for copy in unit_stores(rounded, outs, sem, slot, places(n), every):
                copy.wait()

        multiply_unit(tokens(n, slot), weights, rounded, slot, lambda js: unit_stores(rounded, outs, sem, slot, places(n), js))
        return 0

    lax.fori_loop(0, n_units, body, 0)
    for n in range(max(n_units - 2, 0), n_units):
        for copy in unit_stores(rounded, outs, sem, n % 2, places(n), every):
            copy.wait()


def project_hbm_kernel(plan, *refs):
    arrays, weights = refs[: len(plan)], refs[len(plan) : len(plan) + 2]
    *outs, rounded, out_sem, rows, in_sem = refs[-6:]
    seq = arrays[0].shape[1]
    me = lax.axis_index("tp")
    flat = [(a, e, first + e, mask) for a, (n, first, mask) in enumerate(plan) for e in range(n)]
    units = [flat[k : k + 2] for k in range(0, len(flat), 2)]

    def load(n, slot):
        for k, unit in enumerate(units):

            @pl.when(n == k)
            def _():
                for g, (a, e, _, _) in enumerate(unit):
                    pltpu.make_async_copy(arrays[a].at[e], rows.at[slot, pl.ds(g * seq, seq)], in_sem.at[slot, g]).start()

    def prefetch(n, slot):
        for g in range(2):
            pltpu.make_async_copy(arrays[0].at[0], rows.at[slot, pl.ds(g * seq, seq)], in_sem.at[slot, g]).wait()

        @pl.when(n + 1 < len(units))
        def _():
            load(n + 1, 1 - slot)

    def places(n):
        return [(pick(n, [u[g][2] for u in units]), me ^ pick(n, [u[g][3] for u in units])) for g in range(2)]

    load(0, 0)
    run_units(len(units), prefetch, lambda n, slot: rows[slot], weights, outs, rounded, out_sem, places)


def project_vmem_kernel(plan, *refs):
    arrays, weights = refs[: len(plan)], refs[len(plan) : len(plan) + 2]
    *outs, rounded, out_sem = refs[-4:]
    me = lax.axis_index("tp")
    run_units(
        plan[0][0],
        lambda n, slot: None,
        lambda n, slot: jnp.concatenate([a[n] for a in arrays], axis=0),
        weights,
        outs,
        rounded,
        out_sem,
        lambda n: [(first + n, me ^ mask) for _, first, mask in plan],
    )


def project(in_vmem, vmem_mib, arrays, plan, weights, caches, cache_shape):
    n_arrays = len(arrays)
    n_layers, width, columns = weights[0].shape
    seq = arrays[0].shape[1]
    entries = sum(n for n, _, _ in plan)
    if in_vmem:
        arrays = [pltpu.with_memory_space_constraint(a, pltpu.VMEM) for a in arrays]
    elif caches:
        arrays = [pltpu.with_memory_space_constraint(a, pltpu.HBM) for a in arrays]
    weights = [pltpu.with_memory_space_constraint(w, pltpu.VMEM) for w in weights]
    scratch = [pltpu.VMEM((2, 2 * n_layers, 2 * seq * columns // 128, 128), jnp.bfloat16), pltpu.SemaphoreType.DMA((2, 2 * n_layers, 2))]
    if not in_vmem:
        scratch += [pltpu.VMEM((2, 2 * seq, width), jnp.bfloat16), pltpu.SemaphoreType.DMA((2, 2))]
    return pl.pallas_call(
        functools.partial(project_vmem_kernel if in_vmem else project_hbm_kernel, plan),
        out_shape=[jax.ShapeDtypeStruct(cache_shape, jnp.bfloat16)] * 2,
        in_specs=[VMEM if in_vmem else HBM] * n_arrays + [VMEM, VMEM] + [HBM] * len(caches),
        out_specs=[HBM, HBM],
        input_output_aliases={n_arrays + 2 + i: i for i in range(len(caches))},
        scratch_shapes=scratch,
        compiler_params=pltpu.CompilerParams(vmem_limit_bytes=vmem_mib * 2**20),
        cost_estimate=pl.CostEstimate(
            flops=2 * entries * seq * width * columns * 2 * n_layers,
            bytes_accessed=2 * entries * seq * (width + columns * 2 * n_layers),
            transcendentals=0,
        ),
    )(*arrays, *weights, *caches)


def solution(mesh):
    def per_device(enc_out, norm_scale, w_key, w_value):
        n_batch, seq, _ = enc_out.shape
        n_layers, _, heads, head_dim = w_key.shape
        n_dev = mesh.shape["tp"]

        def swap(a, mask):
            return lax.ppermute(a, "tp", [(i, i ^ mask) for i in range(n_dev)])

        first = [sum(PIECES[:k]) for k in range(len(PIECES))]
        half = sum(PIECES)
        spans = [[(n, s * half + f) for f, n in zip(first, PIECES)] for s in (0, 1)]
        own = [list(ys) for ys in zip(prepare(enc_out, norm_scale, [(spans[s][0][1], PIECES[0]) for s in (0, 1)]))]
        rest = [(spans[s][k][1], n) for k, n in enumerate(PIECES) if k for s in (0, 1)]
        own[0][0], own[1][0], enc_out = together(own[0][0], own[1][0], enc_out)
        *ys, w_key, w_value = prepare(enc_out, norm_scale, rest, (w_key, w_value))
        weights = [w_key, w_value]
        for k in range(len(rest) // 2):
            for s in (0, 1):
                own[s].append(ys[2 * k + s])

        arrived = {}

        def send(what):
            for link, mask in ((0, NEAR_X), (1, NEAR_Y)):
                kind, k = what[0], int(what[1])
                if kind == "f":
                    array, span, _ = arrived[1 - link, f"a{k}"]
                    arrived[link, what] = [swap(array, mask), span, DIAGONAL]
                else:
                    s = link if kind == "a" else 1 - link
                    arrived[link, what] = [swap(own[s][k], mask), spans[s][k], mask]

        def to_partner(group):
            return [[swap(a, CORE), span, mask ^ CORE] for a, span, mask in group]

        for what in ORDER:
            if what[0] != "f":
                send(what)
        mine = [[own[s][k], spans[s][k], 0] for k in range(len(PIECES)) for s in (0, 1)]
        theirs = to_partner(mine)
        cache_shape = (n_layers, n_batch, n_dev * seq * heads, head_dim)

        def call(in_vmem, vmem_mib, group, caches):
            return project(in_vmem, vmem_mib, [a for a, _, _ in group], [(*span, mask) for _, span, mask in group], weights, caches, cache_shape)

        caches = call(False, 57, mine + theirs, ())
        left = []
        for what in ORDER:
            group = [arrived[link, what] for link in (0, 1)]
            group[0][0], group[1][0], *caches = together(group[0][0], group[1][0], *caches)
            if what[0] == "a":
                send("f" + what[1])
            swapped = to_partner(group)
            caches = call(False, 24, left + group, caches)
            left = swapped if what in JOINED else []
            if not left:
                caches = call(True, 24, swapped, caches)
        return tuple(c.reshape(n_layers, n_batch, n_dev * seq, heads, head_dim) for c in caches)

    weight_spec = P(None, None, "tp", None)
    cache_spec = P(None, "dp", None, "tp", None)
    return jax.shard_map(per_device, mesh=mesh, in_specs=(P("dp", "tp", None), P(None), weight_spec, weight_spec), out_specs=(cache_spec, cache_spec), check_vma=False)
```

```python
import functools

import jax
import jax.numpy as jnp
from jax import lax
from jax.experimental import pallas as pl
from jax.experimental.pallas import tpu as pltpu
from jax.sharding import PartitionSpec as P


NORM_EPS = 1e-6

CORE, NEAR_X, NEAR_Y, DIAGONAL = 1, 2, 4, 6
PIECES = (4, 2)
ORDER = ("a0", "b0", "f0", "a1", "b1", "f1")
JOINED = ()

HBM = pl.BlockSpec(memory_space=pltpu.HBM)
VMEM = pl.BlockSpec(memory_space=pltpu.VMEM)


def rms_norm(enc_out, norm_scale):
    acts = enc_out.astype(jnp.float32)
    mean_sq = jnp.mean(acts * acts, axis=-1, keepdims=True)
    return (acts * lax.rsqrt(mean_sq + NORM_EPS) * norm_scale.astype(jnp.float32)).astype(jnp.bfloat16)


def prepare_kernel(pieces, has_weights, *refs):
    enc_out, norm_scale, *refs = refs
    entries = [(p, e, first + e) for p, (first, n) in enumerate(pieces) for e in range(n)]
    if has_weights:
        w_in, refs = refs[:2], refs[2:]
    outs, refs = refs[: len(pieces)], refs[len(pieces) :]
    if has_weights:
        w_out, refs = refs[:2], refs[2:]
    x, y, scale, in_sem, out_sem, scale_sem, *refs = refs
    load_scale = pltpu.make_async_copy(norm_scale, scale, scale_sem)
    load_scale.start()
    loads = [pltpu.make_async_copy(enc_out.at[b], x.at[k], in_sem.at[k]) for k, (_, _, b) in enumerate(entries)]
    stores = [pltpu.make_async_copy(y.at[k], outs[p].at[e], out_sem.at[k]) for k, (p, e, _) in enumerate(entries)]
    starts = [sum(n for _, n in pieces[:p]) for p in range(len(pieces))]
    for copy in loads:
        copy.start()
    w_loads = []
    if has_weights:
        w_raw, w_sem = refs
        n_layers = w_raw.shape[1]
        w_loads = [(i, l, pltpu.make_async_copy(w_in[i].at[l], w_raw.at[i, l], w_sem.at[i, l])) for l in range(n_layers) for i in (0, 1)]
    for _, _, copy in w_loads:
        copy.start()
    load_scale.wait()

    for p, (_, n) in enumerate(pieces):

        def normalize(e, _):
            k = starts[p] + e
            pltpu.make_async_copy(enc_out.at[0], x.at[k], in_sem.at[k]).wait()
            if has_weights:
                y[k] = rms_norm(x[k], scale[...])
                pltpu.make_async_copy(y.at[k], outs[p].at[e], out_sem.at[k]).start()
            else:
                outs[p][e] = rms_norm(x[k], scale[...])
            return 0

        lax.fori_loop(0, n, normalize, 0)
    if has_weights:

        def lay_out(l, _):
            for i in (0, 1):
                pltpu.make_async_copy(w_in[i].at[l], w_raw.at[i, l], w_sem.at[i, l]).wait()


            def some_rows(r, _):
                at = pl.ds(pl.multiple_of(r * 256, 256), 256)
                for i in (0, 1):
                    w_out[i][l, at] = w_raw[i, l, at].reshape(256, w_out[i].shape[2])
                return 0

            lax.fori_loop(0, w_raw.shape[2] // 256, some_rows, 0)
            return 0

        lax.fori_loop(0, n_layers, lay_out, 0)
        for store in stores:
            store.wait()


def prepare(enc_out, norm_scale, pieces, weights=()):
    _, seq, width = enc_out.shape
    n = sum(n for _, n in pieces)
    out_shape = [jax.ShapeDtypeStruct((n, seq, width), jnp.bfloat16) for _, n in pieces]
    scratch = [pltpu.VMEM((n, seq, width), jnp.bfloat16)] * 2 + [pltpu.VMEM((width,), jnp.bfloat16)]
    scratch += [pltpu.SemaphoreType.DMA((n,))] * 2 + [pltpu.SemaphoreType.DMA]
    for w in weights[:1]:
        n_layers, _, heads, head_dim = w.shape
        out_shape += [jax.ShapeDtypeStruct((n_layers, width, heads * head_dim), jnp.bfloat16)] * 2
        scratch += [pltpu.VMEM((2, *w.shape), jnp.bfloat16), pltpu.SemaphoreType.DMA((2, n_layers))]
    return pl.pallas_call(
        functools.partial(prepare_kernel, pieces, bool(weights)),
        out_shape=out_shape,
        in_specs=[HBM] * (2 + len(weights)),
        out_specs=[HBM if weights else VMEM] * len(pieces) + [VMEM] * len(weights),
        scratch_shapes=scratch,
        compiler_params=pltpu.CompilerParams(vmem_limit_bytes=(32 if weights else 18) * 2**20),
        cost_estimate=pl.CostEstimate(flops=8 * n * seq * width, bytes_accessed=4 * n * seq * width, transcendentals=0),
    )(*[pltpu.with_memory_space_constraint(a, pltpu.HBM) for a in (enc_out, norm_scale, *weights)])


def together(*values):
    return lax.optimization_barrier(values)


def pick(n, values):
    out = values[-1]
    for k in range(len(values) - 2, -1, -1):
        out = jnp.where(n == k, values[k], out)
    return out


def multiply_unit(x, weights, rounded, slot, stores):
    for j in range(rounded.shape[1]):
        product = jnp.dot(x, weights[j % 2][j // 2], preferred_element_type=jnp.float32)
        rounded[slot, j] = product.reshape(rounded.shape[2:]).astype(jnp.bfloat16)
        for copy in stores([j]):
            copy.start()


def unit_stores(rounded, outs, sem, slot, places, matrices):
    rows = rounded.shape[2] // len(places)
    for g, (entry, source) in enumerate(places):
        for j in matrices:
            to = outs[j % 2].at[j // 2, entry, pl.ds(pl.multiple_of(source * rows, rows), rows)]
            yield pltpu.make_async_copy(rounded.at[slot, j, pl.ds(g * rows, rows)], to, sem.at[slot, j, g])


def run_units(n_units, prefetch, tokens, weights, outs, rounded, sem, places):
    every = range(rounded.shape[1])

    def body(n, _):
        slot = lax.rem(n, 2)
        prefetch(n, slot)

        @pl.when(n >= 2)
        def _():
            for copy in unit_stores(rounded, outs, sem, slot, places(n), every):
                copy.wait()

        multiply_unit(tokens(n, slot), weights, rounded, slot, lambda js: unit_stores(rounded, outs, sem, slot, places(n), js))
        return 0

    lax.fori_loop(0, n_units, body, 0)
    for n in range(max(n_units - 2, 0), n_units):
        for copy in unit_stores(rounded, outs, sem, n % 2, places(n), every):
            copy.wait()


def project_hbm_kernel(plan, *refs):
    arrays, weights = refs[: len(plan)], refs[len(plan) : len(plan) + 2]
    *outs, rounded, out_sem, rows, in_sem = refs[-6:]
    seq = arrays[0].shape[1]
    me = lax.axis_index("tp")
    flat = [(a, e, first + e, mask) for a, (n, first, mask) in enumerate(plan) for e in range(n)]
    units = [flat[k : k + 2] for k in range(0, len(flat), 2)]

    def load(n, slot):
        for k, unit in enumerate(units):

            @pl.when(n == k)
            def _():
                for g, (a, e, _, _) in enumerate(unit):
                    pltpu.make_async_copy(arrays[a].at[e], rows.at[slot, pl.ds(g * seq, seq)], in_sem.at[slot, g]).start()

    def prefetch(n, slot):
        for g in range(2):
            pltpu.make_async_copy(arrays[0].at[0], rows.at[slot, pl.ds(g * seq, seq)], in_sem.at[slot, g]).wait()

        @pl.when(n + 1 < len(units))
        def _():
            load(n + 1, 1 - slot)

    def places(n):
        return [(pick(n, [u[g][2] for u in units]), me ^ pick(n, [u[g][3] for u in units])) for g in range(2)]

    load(0, 0)
    run_units(len(units), prefetch, lambda n, slot: rows[slot], weights, outs, rounded, out_sem, places)


def project_vmem_kernel(plan, *refs):
    arrays, weights = refs[: len(plan)], refs[len(plan) : len(plan) + 2]
    *outs, rounded, out_sem = refs[-4:]
    me = lax.axis_index("tp")
    run_units(
        plan[0][0],
        lambda n, slot: None,
        lambda n, slot: jnp.concatenate([a[n] for a in arrays], axis=0),
        weights,
        outs,
        rounded,
        out_sem,
        lambda n: [(first + n, me ^ mask) for _, first, mask in plan],
    )


def project(in_vmem, vmem_mib, arrays, plan, weights, caches, cache_shape):
    n_arrays = len(arrays)
    n_layers, width, columns = weights[0].shape
    seq = arrays[0].shape[1]
    entries = sum(n for n, _, _ in plan)
    if in_vmem:
        arrays = [pltpu.with_memory_space_constraint(a, pltpu.VMEM) for a in arrays]
    else:
        arrays = [pltpu.with_memory_space_constraint(a, pltpu.HBM) for a in arrays]
    weights = [pltpu.with_memory_space_constraint(w, pltpu.VMEM) for w in weights]
    scratch = [pltpu.VMEM((2, 2 * n_layers, 2 * seq * columns // 128, 128), jnp.bfloat16), pltpu.SemaphoreType.DMA((2, 2 * n_layers, 2))]
    if not in_vmem:
        scratch += [pltpu.VMEM((2, 2 * seq, width), jnp.bfloat16), pltpu.SemaphoreType.DMA((2, 2))]
    return pl.pallas_call(
        functools.partial(project_vmem_kernel if in_vmem else project_hbm_kernel, plan),
        out_shape=[jax.ShapeDtypeStruct(cache_shape, jnp.bfloat16)] * 2,
        in_specs=[VMEM if in_vmem else HBM] * n_arrays + [VMEM, VMEM] + [HBM] * len(caches),
        out_specs=[HBM, HBM],
        input_output_aliases={n_arrays + 2 + i: i for i in range(len(caches))},
        scratch_shapes=scratch,
        compiler_params=pltpu.CompilerParams(vmem_limit_bytes=vmem_mib * 2**20),
        cost_estimate=pl.CostEstimate(
            flops=2 * entries * seq * width * columns * 2 * n_layers,
            bytes_accessed=2 * entries * seq * (width + columns * 2 * n_layers),
            transcendentals=0,
        ),
    )(*arrays, *weights, *caches)


def solution(mesh):
    def per_device(enc_out, norm_scale, w_key, w_value):
        n_batch, seq, _ = enc_out.shape
        n_layers, _, heads, head_dim = w_key.shape
        n_dev = mesh.shape["tp"]

        def swap(a, mask):
            return lax.ppermute(a, "tp", [(i, i ^ mask) for i in range(n_dev)])

        first = [sum(PIECES[:k]) for k in range(len(PIECES))]
        half = sum(PIECES)
        spans = [[(n, s * half + f) for f, n in zip(first, PIECES)] for s in (0, 1)]
        own = [list(ys) for ys in zip(prepare(enc_out, norm_scale, [(spans[s][0][1], PIECES[0]) for s in (0, 1)]))]
        rest = [(spans[s][k][1], n) for k, n in enumerate(PIECES) if k for s in (0, 1)]
        own[0][0], own[1][0], enc_out = together(own[0][0], own[1][0], enc_out)
        *ys, w_key, w_value = prepare(enc_out, norm_scale, rest, (w_key, w_value))
        weights = [w_key, w_value]
        for k in range(len(rest) // 2):
            for s in (0, 1):
                own[s].append(ys[2 * k + s])

        arrived = {}

        def send(what):
            for link, mask in ((0, NEAR_X), (1, NEAR_Y)):
                kind, k = what[0], int(what[1])
                if kind == "f":
                    array, span, _ = arrived[1 - link, f"a{k}"]
                    arrived[link, what] = [swap(array, mask), span, DIAGONAL]
                else:
                    s = link if kind == "a" else 1 - link
                    arrived[link, what] = [swap(own[s][k], mask), spans[s][k], mask]

        def to_partner(group):
            return [[swap(a, CORE), span, mask ^ CORE] for a, span, mask in group]

        for what in ORDER:
            if what[0] != "f":
                send(what)
        mine = [[own[s][k], spans[s][k], 0] for k in range(len(PIECES)) for s in (0, 1)]
        theirs = to_partner(mine)
        cache_shape = (n_layers, n_batch, n_dev * seq * heads, head_dim)

        def call(in_vmem, vmem_mib, group, caches):
            return project(in_vmem, vmem_mib, [a for a, _, _ in group], [(*span, mask) for _, span, mask in group], weights, caches, cache_shape)

        caches = call(False, 24, mine + theirs, ())
        left = []
        for what in ORDER:
            group = [arrived[link, what] for link in (0, 1)]
            group[0][0], group[1][0], *caches = together(group[0][0], group[1][0], *caches)
            if what[0] == "a":
                send("f" + what[1])
            swapped = to_partner(group)
            caches = call(False, 24, left + group, caches)
            left = swapped if what in JOINED else []
            if not left:
                caches = call(True, 24, swapped, caches)
        return tuple(c.reshape(n_layers, n_batch, n_dev * seq, heads, head_dim) for c in caches)

    weight_spec = P(None, None, "tp", None)
    cache_spec = P(None, "dp", None, "tp", None)
    return jax.shard_map(per_device, mesh=mesh, in_specs=(P("dp", "tp", None), P(None), weight_spec, weight_spec), out_specs=(cache_spec, cache_spec), check_vma=False)
```

```python
import functools

import jax
import jax.numpy as jnp
from jax import lax
from jax.experimental import pallas as pl
from jax.experimental.pallas import tpu as pltpu
from jax.sharding import PartitionSpec as P


NORM_EPS = 1e-6

CORE, NEAR_X, NEAR_Y, DIAGONAL = 1, 2, 4, 6
PIECES = (4, 2)
ORDER = ("a0", "b0", "f0", "a1", "b1", "f1")
JOINED = ("a0",)
IN_VMEM = ("b0", "f0")

HBM = pl.BlockSpec(memory_space=pltpu.HBM)
VMEM = pl.BlockSpec(memory_space=pltpu.VMEM)


def rms_norm(enc_out, norm_scale):
    acts = enc_out.astype(jnp.float32)
    mean_sq = jnp.mean(acts * acts, axis=-1, keepdims=True)
    return (acts * lax.rsqrt(mean_sq + NORM_EPS) * norm_scale.astype(jnp.float32)).astype(jnp.bfloat16)


def prepare_kernel(pieces, has_weights, *refs):
    enc_out, norm_scale, *refs = refs
    entries = [(p, e, first + e) for p, (first, n) in enumerate(pieces) for e in range(n)]
    if has_weights:
        w_in, refs = refs[:2], refs[2:]
    outs, refs = refs[: len(pieces)], refs[len(pieces) :]
    if has_weights:
        w_out, refs = refs[:2], refs[2:]
    x, y, scale, in_sem, out_sem, scale_sem, *refs = refs
    load_scale = pltpu.make_async_copy(norm_scale, scale, scale_sem)
    load_scale.start()
    loads = [pltpu.make_async_copy(enc_out.at[b], x.at[k], in_sem.at[k]) for k, (_, _, b) in enumerate(entries)]
    stores = [pltpu.make_async_copy(y.at[k], outs[p].at[e], out_sem.at[k]) for k, (p, e, _) in enumerate(entries)]
    starts = [sum(n for _, n in pieces[:p]) for p in range(len(pieces))]
    for copy in loads:
        copy.start()
    w_loads = []
    if has_weights:
        w_raw, w_sem = refs
        n_layers = w_raw.shape[1]
        w_loads = [(i, l, pltpu.make_async_copy(w_in[i].at[l], w_raw.at[i, l], w_sem.at[i, l])) for l in range(n_layers) for i in (0, 1)]
    for _, _, copy in w_loads:
        copy.start()
    load_scale.wait()

    for p, (_, n) in enumerate(pieces):

        def normalize(e, _):
            k = starts[p] + e
            pltpu.make_async_copy(enc_out.at[0], x.at[k], in_sem.at[k]).wait()
            if has_weights:
                y[k] = rms_norm(x[k], scale[...])
                pltpu.make_async_copy(y.at[k], outs[p].at[e], out_sem.at[k]).start()
            else:
                outs[p][e] = rms_norm(x[k], scale[...])
            return 0

        lax.fori_loop(0, n, normalize, 0)
    if has_weights:

        def lay_out(l, _):
            for i in (0, 1):
                pltpu.make_async_copy(w_in[i].at[l], w_raw.at[i, l], w_sem.at[i, l]).wait()


            def some_rows(r, _):
                at = pl.ds(pl.multiple_of(r * 256, 256), 256)
                for i in (0, 1):
                    w_out[i][l, at] = w_raw[i, l, at].reshape(256, w_out[i].shape[2])
                return 0

            lax.fori_loop(0, w_raw.shape[2] // 256, some_rows, 0)
            return 0

        lax.fori_loop(0, n_layers, lay_out, 0)
        for store in stores:
            store.wait()


def prepare(enc_out, norm_scale, pieces, weights=()):
    _, seq, width = enc_out.shape
    n = sum(n for _, n in pieces)
    out_shape = [jax.ShapeDtypeStruct((n, seq, width), jnp.bfloat16) for _, n in pieces]
    scratch = [pltpu.VMEM((n, seq, width), jnp.bfloat16)] * 2 + [pltpu.VMEM((width,), jnp.bfloat16)]
    scratch += [pltpu.SemaphoreType.DMA((n,))] * 2 + [pltpu.SemaphoreType.DMA]
    for w in weights[:1]:
        n_layers, _, heads, head_dim = w.shape
        out_shape += [jax.ShapeDtypeStruct((n_layers, width, heads * head_dim), jnp.bfloat16)] * 2
        scratch += [pltpu.VMEM((2, *w.shape), jnp.bfloat16), pltpu.SemaphoreType.DMA((2, n_layers))]
    return pl.pallas_call(
        functools.partial(prepare_kernel, pieces, bool(weights)),
        out_shape=out_shape,
        in_specs=[HBM] * (2 + len(weights)),
        out_specs=[HBM if weights else VMEM] * len(pieces) + [VMEM] * len(weights),
        scratch_shapes=scratch,
        compiler_params=pltpu.CompilerParams(vmem_limit_bytes=(32 if weights else 18) * 2**20),
        cost_estimate=pl.CostEstimate(flops=8 * n * seq * width, bytes_accessed=4 * n * seq * width, transcendentals=0),
    )(*[pltpu.with_memory_space_constraint(a, pltpu.HBM) for a in (enc_out, norm_scale, *weights)])


def together(*values):
    return lax.optimization_barrier(values)


def pick(n, values):
    out = values[-1]
    for k in range(len(values) - 2, -1, -1):
        out = jnp.where(n == k, values[k], out)
    return out


def multiply_unit(x, weights, rounded, slot, stores):
    for j in range(rounded.shape[1]):
        product = jnp.dot(x, weights[j % 2][j // 2], preferred_element_type=jnp.float32)
        rounded[slot, j] = product.reshape(rounded.shape[2:]).astype(jnp.bfloat16)
        for copy in stores([j]):
            copy.start()


def unit_stores(rounded, outs, sem, slot, places, matrices):
    rows = rounded.shape[2] // len(places)
    for g, (entry, source) in enumerate(places):
        for j in matrices:
            to = outs[j % 2].at[j // 2, entry, pl.ds(pl.multiple_of(source * rows, rows), rows)]
            yield pltpu.make_async_copy(rounded.at[slot, j, pl.ds(g * rows, rows)], to, sem.at[slot, j, g])


def run_units(n_units, prefetch, tokens, weights, outs, rounded, sem, places):
    every = range(rounded.shape[1])

    def body(n, _):
        slot = lax.rem(n, 2)
        prefetch(n, slot)

        @pl.when(n >= 2)
        def _():
            for copy in unit_stores(rounded, outs, sem, slot, places(n), every):
                copy.wait()

        multiply_unit(tokens(n, slot), weights, rounded, slot, lambda js: unit_stores(rounded, outs, sem, slot, places(n), js))
        return 0

    lax.fori_loop(0, n_units, body, 0)
    for n in range(max(n_units - 2, 0), n_units):
        for copy in unit_stores(rounded, outs, sem, n % 2, places(n), every):
            copy.wait()


def project_hbm_kernel(plan, *refs):
    arrays, weights = refs[: len(plan)], refs[len(plan) : len(plan) + 2]
    *outs, rounded, out_sem, rows, in_sem = refs[-6:]
    seq = arrays[0].shape[1]
    me = lax.axis_index("tp")
    flat = [(a, e, first + e, mask) for a, (n, first, mask) in enumerate(plan) for e in range(n)]
    units = [flat[k : k + 2] for k in range(0, len(flat), 2)]

    def load(n, slot):
        for k, unit in enumerate(units):

            @pl.when(n == k)
            def _():
                for g, (a, e, _, _) in enumerate(unit):
                    pltpu.make_async_copy(arrays[a].at[e], rows.at[slot, pl.ds(g * seq, seq)], in_sem.at[slot, g]).start()

    def prefetch(n, slot):
        for g in range(2):
            pltpu.make_async_copy(arrays[0].at[0], rows.at[slot, pl.ds(g * seq, seq)], in_sem.at[slot, g]).wait()

        @pl.when(n + 1 < len(units))
        def _():
            load(n + 1, 1 - slot)

    def places(n):
        return [(pick(n, [u[g][2] for u in units]), me ^ pick(n, [u[g][3] for u in units])) for g in range(2)]

    load(0, 0)
    run_units(len(units), prefetch, lambda n, slot: rows[slot], weights, outs, rounded, out_sem, places)


def project_vmem_kernel(plan, *refs):
    arrays, weights = refs[: len(plan)], refs[len(plan) : len(plan) + 2]
    *outs, rounded, out_sem = refs[-4:]
    me = lax.axis_index("tp")
    run_units(
        plan[0][0],
        lambda n, slot: None,
        lambda n, slot: jnp.concatenate([a[n] for a in arrays], axis=0),
        weights,
        outs,
        rounded,
        out_sem,
        lambda n: [(first + n, me ^ mask) for _, first, mask in plan],
    )


def project(in_vmem, vmem_mib, arrays, plan, weights, caches, cache_shape):
    n_arrays = len(arrays)
    n_layers, width, columns = weights[0].shape
    seq = arrays[0].shape[1]
    entries = sum(n for n, _, _ in plan)
    if in_vmem:
        arrays = [pltpu.with_memory_space_constraint(a, pltpu.VMEM) for a in arrays]
    else:
        arrays = [pltpu.with_memory_space_constraint(a, pltpu.HBM) for a in arrays]
    weights = [pltpu.with_memory_space_constraint(w, pltpu.VMEM) for w in weights]
    scratch = [pltpu.VMEM((2, 2 * n_layers, 2 * seq * columns // 128, 128), jnp.bfloat16), pltpu.SemaphoreType.DMA((2, 2 * n_layers, 2))]
    if not in_vmem:
        scratch += [pltpu.VMEM((2, 2 * seq, width), jnp.bfloat16), pltpu.SemaphoreType.DMA((2, 2))]
    return pl.pallas_call(
        functools.partial(project_vmem_kernel if in_vmem else project_hbm_kernel, plan),
        out_shape=[jax.ShapeDtypeStruct(cache_shape, jnp.bfloat16)] * 2,
        in_specs=[VMEM if in_vmem else HBM] * n_arrays + [VMEM, VMEM] + [HBM] * len(caches),
        out_specs=[HBM, HBM],
        input_output_aliases={n_arrays + 2 + i: i for i in range(len(caches))},
        scratch_shapes=scratch,
        compiler_params=pltpu.CompilerParams(vmem_limit_bytes=vmem_mib * 2**20),
        cost_estimate=pl.CostEstimate(
            flops=2 * entries * seq * width * columns * 2 * n_layers,
            bytes_accessed=2 * entries * seq * (width + columns * 2 * n_layers),
            transcendentals=0,
        ),
    )(*arrays, *weights, *caches)


def solution(mesh):
    def per_device(enc_out, norm_scale, w_key, w_value):
        n_batch, seq, _ = enc_out.shape
        n_layers, _, heads, head_dim = w_key.shape
        n_dev = mesh.shape["tp"]

        def swap(a, mask):
            return lax.ppermute(a, "tp", [(i, i ^ mask) for i in range(n_dev)])

        first = [sum(PIECES[:k]) for k in range(len(PIECES))]
        half = sum(PIECES)
        spans = [[(n, s * half + f) for f, n in zip(first, PIECES)] for s in (0, 1)]
        own = [list(ys) for ys in zip(prepare(enc_out, norm_scale, [(spans[s][0][1], PIECES[0]) for s in (0, 1)]))]
        rest = [(spans[s][k][1], n) for k, n in enumerate(PIECES) if k for s in (0, 1)]
        own[0][0], own[1][0], enc_out = together(own[0][0], own[1][0], enc_out)
        *ys, w_key, w_value = prepare(enc_out, norm_scale, rest, (w_key, w_value))
        weights = [w_key, w_value]
        for k in range(len(rest) // 2):
            for s in (0, 1):
                own[s].append(ys[2 * k + s])

        arrived = {}

        def send(what):
            for link, mask in ((0, NEAR_X), (1, NEAR_Y)):
                kind, k = what[0], int(what[1])
                if kind == "f":
                    array, span, _ = arrived[1 - link, f"a{k}"]
                    arrived[link, what] = [swap(array, mask), span, DIAGONAL]
                else:
                    s = link if kind == "a" else 1 - link
                    arrived[link, what] = [swap(own[s][k], mask), spans[s][k], mask]

        def to_partner(group):
            return [[swap(a, CORE), span, mask ^ CORE] for a, span, mask in group]

        for what in ORDER:
            if what[0] != "f":
                send(what)
        mine = [[own[s][k], spans[s][k], 0] for k in range(len(PIECES)) for s in (0, 1)]
        theirs = to_partner(mine)
        cache_shape = (n_layers, n_batch, n_dev * seq * heads, head_dim)

        def call(in_vmem, vmem_mib, group, caches):
            return project(in_vmem, vmem_mib, [a for a, _, _ in group], [(*span, mask) for _, span, mask in group], weights, caches, cache_shape)

        caches = call(False, 24, mine + theirs, ())
        for what in ORDER:
            group = [arrived[link, what] for link in (0, 1)]
            group[0][0], group[1][0], *caches = together(group[0][0], group[1][0], *caches)
            if what[0] == "a":
                send("f" + what[1])
            swapped = to_partner(group)
            if what in JOINED:
                caches = call(False, 24, group + swapped, caches)
            else:
                caches = call(what in IN_VMEM, 24, group, caches)
                caches = call(True, 24, swapped, caches)
        return tuple(c.reshape(n_layers, n_batch, n_dev * seq, heads, head_dim) for c in caches)

    weight_spec = P(None, None, "tp", None)
    cache_spec = P(None, "dp", None, "tp", None)
    return jax.shard_map(per_device, mesh=mesh, in_specs=(P("dp", "tp", None), P(None), weight_spec, weight_spec), out_specs=(cache_spec, cache_spec), check_vma=False)
```
